32 devices in a mesh: replica: 8 (over z, x), model: 4 (over y, core).
Axes of the slice: x: 2, y: 2, z: 4, core: 2. Of those that a mesh axis runs over, the one named last changes fastest.
Arguments:
- grad_up: float32 [8, 1280, 5120], P('replica', None, 'model'), may hold values from -4 to 4
- grad_down: float32 [8, 5120, 1280], P('replica', 'model'), may hold values from -4 to 4
- grad_query: float32 [8, 1280, 1280], P('replica', None, 'model'), may hold values from -4 to 4
- grad_key: float32 [8, 1280, 1280], P('replica', None, 'model'), may hold values from -4 to 4
- grad_value: float32 [8, 1280, 1280], P('replica', None, 'model'), may hold values from -4 to 4
- grad_mixed: float32 [8, 1280, 1280], P('replica', 'model'), may hold values from -4 to 4
- grad_norm: float32 [8, 1280], P('replica'), may hold values from -8 to 8
- weight_up: float32 [1280, 5120], P('replica', 'model'), may hold values from -0.15625 to 0.15625
- weight_down: float32 [5120, 1280], P('model', 'replica'), may hold values from -0.078125 to 0.078125
- weight_query: float32 [1280, 1280], P('replica', 'model'), may hold values from -0.15625 to 0.15625
- weight_key: float32 [1280, 1280], P('replica', 'model'), may hold values from -0.15625 to 0.15625
- weight_value: float32 [1280, 1280], P('replica', 'model'), may hold values from -0.15625 to 0.15625
- weight_mixed: float32 [1280, 1280], P('model', 'replica'), may hold values from -0.15625 to 0.15625
- weight_norm: float32 [1280], P('replica'), may hold values from 0.25 to 1.75
- moment_up: float32 [1280, 5120], P('replica', 'model'), may hold values from 0.05 to 0.8
- moment_down: float32 [5120, 1280], P('model', 'replica'), may hold values from 0.05 to 0.8
- moment_query: float32 [1280, 1280], P('replica', 'model'), may hold values from 0.05 to 0.8
- moment_key: float32 [1280, 1280], P('replica', 'model'), may hold values from 0.05 to 0.8
- moment_value: float32 [1280, 1280], P('replica', 'model'), may hold values from 0.05 to 0.8
- moment_mixed: float32 [1280, 1280], P('model', 'replica'), may hold values from 0.05 to 0.8
- moment_norm: float32 [1280], P('replica'), may hold values from 0.05 to 0.8
Outputs:
- copy_up: bfloat16 [1280, 5120], P(None, 'model')
- copy_down: bfloat16 [5120, 1280], P('model')
- copy_query: bfloat16 [1280, 1280], P(None, 'model')
- copy_key: bfloat16 [1280, 1280], P(None, 'model')
- copy_value: bfloat16 [1280, 1280], P(None, 'model')
- copy_mixed: bfloat16 [1280, 1280], P('model')
- copy_norm: bfloat16 [1280], replicated
- new_up: float32 [1280, 5120], P('replica', 'model')
- new_down: float32 [5120, 1280], P('model', 'replica')
- new_query: float32 [1280, 1280], P('replica', 'model')
- new_key: float32 [1280, 1280], P('replica', 'model')
- new_value: float32 [1280, 1280], P('replica', 'model')
- new_mixed: float32 [1280, 1280], P('model', 'replica')
- new_norm: float32 [1280], P('replica')
- state_new_up: float32 [1280, 5120], P('replica', 'model')
- state_new_down: float32 [5120, 1280], P('model', 'replica')
- state_new_query: float32 [1280, 1280], P('replica', 'model')
- state_new_key: float32 [1280, 1280], P('replica', 'model')
- state_new_value: float32 [1280, 1280], P('replica', 'model')
- state_new_mixed: float32 [1280, 1280], P('model', 'replica')
- state_new_norm: float32 [1280], P('replica')
The draws below stay inside these ranges and needn't reach their ends.
All inputs are finite; a program needn't handle non-finite values.
Results may differ from the reference program's by a relative error of at most 0.0004.
Values may be sent and summed in bfloat16 or wider, within the bound.
A program may use at most 128 MiB of HBM per device.

```python
import jax
import jax.numpy as jnp
from jax import lax

WIDTH = 1280
INNER = 5120
ATTN = 1280
REPLICAS = 8


def with_spikes(array, rng, source, target, blocks, factor):
    def block_of(dim):
        return (jnp.arange(array.shape[dim]) // (array.shape[dim] // blocks)).reshape((-1,) + (1,) * (array.ndim - 1 - dim))

    near = jax.random.permutation(rng, blocks)[block_of(target)]
    far = (block_of(target) + blocks // 2) % blocks
    return jnp.where((block_of(source) == near) | (block_of(source) == far), factor * array, array)


def block_levels(rng, dims, split, low, top_value):
    gain = 1.0
    for axis_at, blocks in split:
        heights = jax.random.uniform(jax.random.fold_in(jax.random.fold_in(rng, 6), axis_at), (blocks,), jnp.float32, low / len(split), top_value / len(split))
        gain = gain * jnp.repeat(jnp.exp(heights), dims[axis_at] // blocks).reshape((-1,) + (1,) * (len(dims) - 1 - axis_at))
    return gain


def noise(rng, extent, deviation, reach, cuts=(), kind=jnp.bfloat16):
    loudness = block_levels(rng, extent, cuts, -0.22, 0.18) if cuts else 1.0
    entries = jax.random.normal(rng, extent, jnp.float32) * deviation * loudness
    return jnp.minimum(jnp.maximum(entries, -reach), reach).astype(kind)


def noise_with(own_key, dims, scale, reach, cuts, heavy, held_as=jnp.bfloat16):
    array = scale * jax.random.normal(own_key, dims, jnp.float32)
    if cuts:
        array = array * block_levels(own_key, dims, cuts, -0.22, 0.18)
    return jnp.clip(with_spikes(array, jax.random.fold_in(own_key, 3), *heavy), -reach, reach).astype(held_as)


def setup_inputs(seed: int = 0) -> dict:
    seeds = jax.random.split(jax.random.key(seed), 22)
    grad_up = noise_with(seeds[0], (REPLICAS, WIDTH, INNER), 0.5, 4.0, ((0, 8), (2, 4)), (0, 1, 8, 2.0), jnp.float32)
    grad_down = noise_with(seeds[1], (REPLICAS, INNER, WIDTH), 0.5, 4.0, ((0, 8), (1, 4)), (0, 2, 8, 2.0), jnp.float32)
    grad_query = noise_with(seeds[2], (REPLICAS, WIDTH, ATTN), 0.5, 4.0, ((0, 8), (2, 4)), (0, 1, 8, 2.0), jnp.float32)
    grad_key = noise_with(seeds[3], (REPLICAS, WIDTH, ATTN), 0.5, 4.0, ((0, 8), (2, 4)), (0, 1, 8, 2.0), jnp.float32)
    grad_value = noise_with(seeds[4], (REPLICAS, WIDTH, ATTN), 0.5, 4.0, ((0, 8), (2, 4)), (0, 1, 8, 2.0), jnp.float32)
    grad_mixed = noise_with(seeds[5], (REPLICAS, ATTN, WIDTH), 0.5, 4.0, ((0, 8), (1, 4)), (0, 2, 8, 2.0), jnp.float32)
    grad_norm = noise_with(seeds[6], (REPLICAS, WIDTH), 1.0, 8.0, ((0, 8),), (0, 1, 8, 2.0), jnp.float32)
    weight_up = noise(seeds[7], (WIDTH, INNER), WIDTH ** -0.5, 0.15625, ((0, 8), (1, 4)), jnp.float32)
    weight_down = noise(seeds[8], (INNER, WIDTH), INNER ** -0.5, 0.078125, ((0, 4), (1, 8)), jnp.float32)
    weight_query = noise(seeds[9], (WIDTH, ATTN), WIDTH ** -0.5, 0.15625, ((0, 8), (1, 4)), jnp.float32)
    weight_key = noise(seeds[10], (WIDTH, ATTN), WIDTH ** -0.5, 0.15625, ((0, 8), (1, 4)), jnp.float32)
    weight_value = noise(seeds[11], (WIDTH, ATTN), WIDTH ** -0.5, 0.15625, ((0, 8), (1, 4)), jnp.float32)
    weight_mixed = noise(seeds[12], (ATTN, WIDTH), ATTN ** -0.5, 0.15625, ((0, 4), (1, 8)), jnp.float32)
    weight_norm = jnp.clip(1.0 + 0.15 * jax.random.normal(seeds[13], (WIDTH,), jnp.float32), 0.25, 1.75)
    moment_up = jnp.clip(0.05 + 0.75 * jax.random.uniform(seeds[14], (WIDTH, INNER), jnp.float32) ** block_levels(seeds[14], (WIDTH, INNER), ((0, 8), (1, 4)), -0.2, 0.2), 0.05, 0.8)
    moment_down = jnp.clip(0.05 + 0.75 * jax.random.uniform(seeds[15], (INNER, WIDTH), jnp.float32) ** block_levels(seeds[15], (INNER, WIDTH), ((0, 4), (1, 8)), -0.2, 0.2), 0.05, 0.8)
    moment_query = jnp.clip(0.05 + 0.75 * jax.random.uniform(seeds[16], (WIDTH, ATTN), jnp.float32) ** block_levels(seeds[16], (WIDTH, ATTN), ((0, 8), (1, 4)), -0.2, 0.2), 0.05, 0.8)
    moment_key = jnp.clip(0.05 + 0.75 * jax.random.uniform(seeds[17], (WIDTH, ATTN), jnp.float32) ** block_levels(seeds[17], (WIDTH, ATTN), ((0, 8), (1, 4)), -0.2, 0.2), 0.05, 0.8)
    moment_value = jnp.clip(0.05 + 0.75 * jax.random.uniform(seeds[18], (WIDTH, ATTN), jnp.float32) ** block_levels(seeds[18], (WIDTH, ATTN), ((0, 8), (1, 4)), -0.2, 0.2), 0.05, 0.8)
    moment_mixed = jnp.clip(0.05 + 0.75 * jax.random.uniform(seeds[19], (ATTN, WIDTH), jnp.float32) ** block_levels(seeds[19], (ATTN, WIDTH), ((0, 4), (1, 8)), -0.2, 0.2), 0.05, 0.8)
    moment_norm = jnp.clip(0.05 + 0.75 * jax.random.uniform(seeds[20], (WIDTH,), jnp.float32) ** block_levels(seeds[20], (WIDTH,), ((0, 8),), -0.2, 0.2), 0.05, 0.8)
    return {"grad_up": grad_up, "grad_down": grad_down, "grad_query": grad_query, "grad_key": grad_key, "grad_value": grad_value, "grad_mixed": grad_mixed, "grad_norm": grad_norm, "weight_up": weight_up, "weight_down": weight_down, "weight_query": weight_query, "weight_key": weight_key, "weight_value": weight_value, "weight_mixed": weight_mixed, "weight_norm": weight_norm, "moment_up": moment_up, "moment_down": moment_down, "moment_query": moment_query, "moment_key": moment_key, "moment_value": moment_value, "moment_mixed": moment_mixed, "moment_norm": moment_norm}


learn_rate = 0.05
hold_rate = 0.9

def reference(grad_up, grad_down, grad_query, grad_key, grad_value, grad_mixed, grad_norm, weight_up, weight_down, weight_query, weight_key, weight_value, weight_mixed, weight_norm, moment_up, moment_down, moment_query, moment_key, moment_value, moment_mixed, moment_norm):
    mean_up = lax.optimization_barrier(jnp.sum(grad_up.astype(jnp.float32), axis=0)) * REPLICAS ** (-0.5)
    mean_down = lax.optimization_barrier(jnp.sum(grad_down.astype(jnp.float32), axis=0)) * REPLICAS ** (-0.5)
    mean_query = lax.optimization_barrier(jnp.sum(grad_query.astype(jnp.float32), axis=0)) * REPLICAS ** (-0.5)
    mean_key = lax.optimization_barrier(jnp.sum(grad_key.astype(jnp.float32), axis=0)) * REPLICAS ** (-0.5)
    mean_value = lax.optimization_barrier(jnp.sum(grad_value.astype(jnp.float32), axis=0)) * REPLICAS ** (-0.5)
    mean_mixed = lax.optimization_barrier(jnp.sum(grad_mixed.astype(jnp.float32), axis=0)) * REPLICAS ** (-0.5)
    mean_norm = lax.optimization_barrier(jnp.sum(grad_norm.astype(jnp.float32), axis=0)) * REPLICAS ** (-0.5)
    state_new_up = hold_rate * moment_up + (1.0 - hold_rate) * mean_up * mean_up
    new_up = weight_up - learn_rate * mean_up * lax.rsqrt(state_new_up + 1e-06)
    state_new_down = hold_rate * moment_down + (1.0 - hold_rate) * mean_down * mean_down
    new_down = weight_down - learn_rate * mean_down * lax.rsqrt(state_new_down + 1e-06)
    state_new_query = hold_rate * moment_query + (1.0 - hold_rate) * mean_query * mean_query
    new_query = weight_query - learn_rate * mean_query * lax.rsqrt(state_new_query + 1e-06)
    state_new_key = hold_rate * moment_key + (1.0 - hold_rate) * mean_key * mean_key
    new_key = weight_key - learn_rate * mean_key * lax.rsqrt(state_new_key + 1e-06)
    state_new_value = hold_rate * moment_value + (1.0 - hold_rate) * mean_value * mean_value
    new_value = weight_value - learn_rate * mean_value * lax.rsqrt(state_new_value + 1e-06)
    state_new_mixed = hold_rate * moment_mixed + (1.0 - hold_rate) * mean_mixed * mean_mixed
    new_mixed = weight_mixed - learn_rate * mean_mixed * lax.rsqrt(state_new_mixed + 1e-06)
    state_new_norm = hold_rate * moment_norm + (1.0 - hold_rate) * mean_norm * mean_norm
    new_norm = weight_norm - learn_rate * mean_norm * lax.rsqrt(state_new_norm + 1e-06)
    copy_up = new_up.astype(jnp.bfloat16)
    copy_down = new_down.astype(jnp.bfloat16)
    copy_query = new_query.astype(jnp.bfloat16)
    copy_key = new_key.astype(jnp.bfloat16)
    copy_value = new_value.astype(jnp.bfloat16)
    copy_mixed = new_mixed.astype(jnp.bfloat16)
    copy_norm = new_norm.astype(jnp.bfloat16)
    return (copy_up, copy_down, copy_query, copy_key, copy_value, copy_mixed, copy_norm, new_up, new_down, new_query, new_key, new_value, new_mixed, new_norm, state_new_up, state_new_down, state_new_query, state_new_key, state_new_value, state_new_mixed, state_new_norm)
```

```python
import functools

import jax
import jax.numpy as jnp
from jax import lax
from jax.experimental import pallas as pl
from jax.experimental.pallas import tpu as pltpu
from jax.sharding import PartitionSpec as P

learn_rate = 0.05
hold_rate = 0.9

MESH = pl.DeviceIdType.MESH
LANES = 128
RING = 4
AHEAD = 2
GATHER_LAG = 2


def apply_rule(total, weight, moment, rate):
    mean = total * rate
    state = hold_rate * moment + (1.0 - hold_rate) * mean * mean
    return weight - learn_rate * mean * lax.rsqrt(state + 1e-06), state


def kernel(A, B, K, T, S, rate, *refs):
    grads, weights, moments = refs[:K], refs[K : 2 * K], refs[2 * K : 3 * K]
    small_in = refs[3 * K]
    outs = refs[3 * K + 1 :]
    copies, news, states = outs[:K], outs[K : 2 * K], outs[2 * K : 3 * K]
    small_out = outs[3 * K]
    (acc, rx, rz, wv, mv, out,
     ld_sem, st_sem, cp_sem, xs, xr, rs, ls, zr, gs, gr, hs, ks, hr,
     ns, nr) = outs[3 * K + 1 :]
    C = K * T * S
    R = acc.shape[2]
    n = A * B
    me = lax.axis_index("replica")
    a, b = me // B, me % B

    def dev(row, col):
        return {"replica": row * B + col}

    def send(src, dst, ssem, rsem, to):
        return pltpu.make_async_remote_copy(
            src_ref=src, dst_ref=dst, send_sem=ssem, recv_sem=rsem,
            device_id=to, device_id_type=MESH,
        )

    def valid(c):
        return jnp.logical_and(c >= 0, c < C)

    def rows_cols(c):
        rest = c % (T * S)
        t, u = rest // S, rest % S
        return (pl.ds(pl.multiple_of(u * R, R), R),
                pl.ds(pl.multiple_of(t * LANES, LANES), LANES))

    def for_matrix(c, fn):
        k = c // (T * S)
        rows, cols = rows_cols(c)
        for i in range(K):
            @pl.when(k == i)
            def _(i=i):
                fn(i, rows, cols)

    barrier = pltpu.get_barrier_semaphore()
    for i in range(1, n):
        pl.semaphore_signal(
            barrier, inc=1, device_id={"replica": (me + i) % n}, device_id_type=MESH
        )
    pl.semaphore_wait(barrier, n - 1)

    def x_copy(i, rows, cols, c, j):
        to = (b + j) % B
        return send(
            grads[i].at[:, to, rows, cols], rx.at[c, j - 1],
            xs.at[c % RING, j - 1], xr.at[c, j - 1], dev(a, to),
        )

    def load(i, rows, cols, c):
        q = c % RING
        return (
            pltpu.make_async_copy(grads[i].at[:, b, rows, cols], acc.at[c], ld_sem.at[q, 0]),
            pltpu.make_async_copy(weights[i].at[rows, cols], wv.at[c], ld_sem.at[q, 1]),
            pltpu.make_async_copy(moments[i].at[rows, cols], mv.at[c], ld_sem.at[q, 2]),
        )

    def begin(c):
        @pl.when(c >= RING)
        def _():
            for j in range(1, B):
                x_copy(0, *rows_cols(0), c - RING, j).wait_send()

        def go(i, rows, cols):
            for j in range(1, B):
                x_copy(i, rows, cols, c, j).start()
            for one in load(i, rows, cols, c):
                one.start()

        for_matrix(c, go)

    def add_first(c):
        for one in load(0, *rows_cols(0), c):
            one.wait()
        for j in range(1, B):
            x_copy(0, *rows_cols(0), c, j).wait_recv()
        for d in range(A):
            total = acc[c, d]
            for j in range(1, B):
                total = total + rx[c, j - 1, d]
            acc[c, d] = total

    def r_copy(c, d):
        return send(acc.at[c, d], rz.at[c, d], rs.at[c % RING, d], zr.at[c, d], dev(a + 1, b))

    def l_copy(c, d):
        slot = jnp.where(a - 1 == d, A, d)
        return send(acc.at[c, d], rz.at[c, slot], ls.at[c % RING, d], zr.at[c, slot], dev(a - 1, b))

    def go_right(c):
        for d in range(A):
            @pl.when(jnp.logical_and(d >= a, a > 0))
            def _(d=d):
                r_copy(c, d).wait_recv()

            @pl.when(jnp.logical_and(d > a, a > 0))
            def _(d=d):
                acc[c, d] = acc[c, d] + rz[c, d]

            @pl.when(d > a)
            def _(d=d):
                @pl.when(c >= RING)
                def _():
                    r_copy(c - RING, d).wait_send()

                r_copy(c, d).start()

    def go_left(c):
        @pl.when(a < A - 1)
        def _():
            send(acc.at[c, 0], rz.at[c, A], ls.at[0, 0], zr.at[c, A], dev(a, b)).wait_recv()

        for d in range(A):
            @pl.when(jnp.logical_and(d < a, a < A - 1))
            def _(d=d):
                send(acc.at[c, d], rz.at[c, d], ls.at[0, d], zr.at[c, d], dev(a, b)).wait_recv()
                acc[c, d] = acc[c, d] + rz[c, d]

            @pl.when(d < a)
            def _(d=d):
                @pl.when(c >= RING)
                def _():
                    l_copy(c - RING, d).wait_send()

                l_copy(c, d).start()

    def g_copy(c, j):
        return send(
            out.at[c, a, b], out.at[c, a, b], gs.at[c % RING, j - 1],
            gr.at[c, j - 1], dev(a, (b + j) % B),
        )

    def h_copy(c, o):
        return send(out.at[c, o], out.at[c, o], hs.at[c % RING, o], hr.at[c, o], dev(a + 1, b))

    def k_copy(c, o):
        return send(out.at[c, o], out.at[c, o], ks.at[c % RING, o], hr.at[c, o], dev(a - 1, b))

    def store(i, rows, cols, c):
        q = c % RING
        return (
            pltpu.make_async_copy(wv.at[c], news[i].at[rows, cols], st_sem.at[q, 0]),
            pltpu.make_async_copy(mv.at[c], states[i].at[rows, cols], st_sem.at[q, 1]),
        )

    def update(c):
        @pl.when(a > 0)
        def _():
            acc[c, a] = acc[c, a] + rz[c, a]

        @pl.when(a < A - 1)
        def _():
            acc[c, a] = acc[c, a] + rz[c, A]

        new, state = apply_rule(acc[c, a], wv[c], mv[c], rate)
        wv[c] = new
        mv[c] = state
        out[c, a, b] = new.astype(jnp.bfloat16)

        @pl.when(c >= RING)
        def _():
            for j in range(1, B):
                g_copy(c - RING, j).wait_send()
            for one in store(0, *rows_cols(0), c - RING):
                one.wait()

        for j in range(1, B):
            g_copy(c, j).start()

        def go(i, rows, cols):
            for one in store(i, rows, cols, c):
                one.start()

        for_matrix(c, go)

    def pass_on(c, o, right, left):
        @pl.when(right)
        def _():
            @pl.when(c >= RING)
            def _():
                h_copy(c - RING, o).wait_send()

            h_copy(c, o).start()

        @pl.when(left)
        def _():
            @pl.when(c >= RING)
            def _():
                k_copy(c - RING, o).wait_send()

            k_copy(c, o).start()

    def spread(c):
        for j in range(1, B):
            g_copy(c, j).wait_recv()
        for o in range(A):
            @pl.when(o == a)
            def _(o=o):
                pass_on(c, o, a < A - 1, a > 0)

    def forward(c, o):
        h_copy(c, o).wait_recv()
        pass_on(
            c, o,
            jnp.logical_and(o < a, a < A - 1),
            jnp.logical_and(o > a, a > 0),
        )

    def put(i, rows, cols, c):
        return pltpu.make_async_copy(
            out.at[c], copies[i].at[:, :, rows, cols], cp_sem.at[c % RING]
        )

    def finish(c):
        @pl.when(c >= RING)
        def _():
            put(0, *rows_cols(0), c - RING).wait()

        for_matrix(c, lambda i, rows, cols: put(i, rows, cols, c).start())

    def n_copy(i):
        return send(
            small_in, small_out.at[me], ns.at[i - 1], nr.at[i - 1],
            {"replica": (me + i) % n},
        )

    for c in range(min(AHEAD, C)):
        begin(c)
    for i in range(1, n):
        n_copy(i).start()
    small_out[me] = small_in[...]

    late = (A - 1) + GATHER_LAG

    def step(s, carry):
        def at(c, fn):
            @pl.when(valid(c))
            def _():
                fn(c)

        @pl.when(s + AHEAD < C)
        def _():
            begin(s + AHEAD)

        at(s, add_first)
        at(s - a, go_right)
        at(s - (A - 1 - a), go_left)
        at(s - (A - 1), update)
        at(s - late, spread)
        for o in range(A):
            c = s - late - jnp.abs(a - o)

            @pl.when(jnp.logical_and(valid(c), o != a))
            def _(o=o, c=c):
                forward(c, o)
        at(s - late - (A - 1), finish)
        return carry

    lax.fori_loop(0, C + late + A - 1, step, 0)

    for c in range(max(0, C - RING), C):
        for j in range(1, B):
            x_copy(0, *rows_cols(0), c, j).wait_send()
            g_copy(c, j).wait_send()
        for one in store(0, *rows_cols(0), c):
            one.wait()
        put(0, *rows_cols(0), c).wait()
        for d in range(A):
            @pl.when(d > a)
            def _(d=d, c=c):
                r_copy(c, d).wait_send()

            @pl.when(d < a)
            def _(d=d, c=c):
                l_copy(c, d).wait_send()

            @pl.when(jnp.logical_and(d <= a, a < A - 1))
            def _(d=d, c=c):
                h_copy(c, d).wait_send()

            @pl.when(jnp.logical_and(d >= a, a > 0))
            def _(d=d, c=c):
                k_copy(c, d).wait_send()
    for i in range(1, n):
        n_copy(i).wait()


def exchange(grads, weights, moments, small, n):
    B = max(k for k in range(1, n + 1) if n % k == 0 and k * k <= n)
    A = n // B
    K = len(grads)
    rows, width = weights[0].shape
    T = width // LANES
    S = 1
    R = rows // S
    C = K * T * S
    grads = [g.reshape(A, B, rows, width) for g in grads]
    dma = pltpu.SemaphoreType.DMA
    anywhere = pl.BlockSpec(memory_space=pltpu.MemorySpace.HBM)
    vmem = pl.BlockSpec(memory_space=pltpu.VMEM)
    f32 = jnp.float32
    res = pl.pallas_call(
        functools.partial(kernel, A, B, K, T, S, n ** (-0.5)),
        out_shape=(
            [jax.ShapeDtypeStruct((A, B, rows, width), jnp.bfloat16)] * K
            + [jax.ShapeDtypeStruct((rows, width), f32)] * (2 * K)
            + [jax.ShapeDtypeStruct((n,) + small.shape, f32)]
        ),
        in_specs=[anywhere] * (3 * K) + [vmem],
        out_specs=[anywhere] * (3 * K) + [vmem],
        scratch_shapes=[
            pltpu.VMEM((C, A, R, LANES), f32),
            pltpu.VMEM((C, B - 1, A, R, LANES), f32),
            pltpu.VMEM((C, A + 1, R, LANES), f32),
            pltpu.VMEM((C, R, LANES), f32),
            pltpu.VMEM((C, R, LANES), f32),
            pltpu.VMEM((C, A, B, R, LANES), jnp.bfloat16),
            dma((RING, 3)), dma((RING, 2)), dma((RING,)),
            dma((RING, B - 1)), dma((C, B - 1)),
            dma((RING, A)), dma((RING, A)), dma((C, A + 1)),
            dma((RING, B - 1)), dma((C, B - 1)),
            dma((RING, A)), dma((RING, A)), dma((C, A)),
            dma((n - 1,)), dma((n - 1,)),
        ],
        compiler_params=pltpu.CompilerParams(
            collective_id=0, has_side_effects=True, vmem_limit_bytes=64 * 1000 * 1000
        ),
        name="exchange",
    )(*grads, *weights, *moments, small)
    copies = [c.reshape(n * rows, width) for c in res[:K]]
    return copies, res[K : 2 * K], res[2 * K : 3 * K], res[3 * K]


def per_device(*args):
    grads = [g[0] for g in args[:7]]
    weights, moments = list(args[7:14]), list(args[14:21])
    n = lax.axis_size("replica")

    def three(arrays):
        up, down, query, key, value, mixed = arrays
        return [up, down.T, jnp.concatenate([query, key, value, mixed.T], axis=1)]

    attn = grads[2].shape[1]

    def six(arrays):
        up, down, rest = arrays
        query, key, value, mixed = (rest[:, i * attn : (i + 1) * attn] for i in range(4))
        return [up, down.T, query, key, value, mixed.T]

    total, own = grads[6].shape[0], weights[6].shape[0]
    small = jnp.concatenate([grads[6], weights[6], moments[6]])
    pad = -small.shape[0] % (8 * LANES)
    small = jnp.pad(small, (0, pad)).reshape(-1, LANES)
    copies, news, states, smalls = exchange(
        three(grads[:6]), three(weights[:6]), three(moments[:6]), small, n
    )
    smalls = smalls.reshape(n, -1)
    norm_new, norm_state = apply_rule(
        jnp.sum(smalls[:, :total], axis=0),
        smalls[:, total : total + own].reshape(-1),
        smalls[:, total + own : total + 2 * own].reshape(-1),
        n ** (-0.5),
    )
    start = lax.axis_index("replica") * own
    mine = lambda v: lax.dynamic_slice_in_dim(v, start, own)
    return (
        *six(copies), norm_new.astype(jnp.bfloat16),
        *six(news), mine(norm_new),
        *six(states), mine(norm_state),
    )


def solution(mesh):
    whole = [P(None, "model"), P("model", None)]
    shard = [P("replica", "model"), P("model", "replica")]
    kinds = [0, 1, 0, 0, 0, 1]
    grads = [P("replica", *whole[k]) for k in kinds] + [P("replica", None)]
    shards = [shard[k] for k in kinds] + [P("replica")]
    gathered = [whole[k] for k in kinds] + [P()]
    return jax.shard_map(
        per_device,
        mesh=mesh,
        in_specs=(*grads, *shards, *shards),
        out_specs=(*gathered, *shards, *shards),
        check_vma=False,
    )
```
